512 devices in a mesh: leaf: 128 (over y, z, core), rep: 4 (over x).
Axes of the slice: x: 4, y: 8, z: 8, core: 2. Of those that a mesh axis runs over, the one named last changes fastest.
Arguments:
- coords: float32 [8, 131072], P(None, 'leaf'), may hold values from -8 to 8
- skeleton: float32 [8, 16384], P(None, 'leaf'), may hold values from -8 to 8
- transfer: bfloat16 [256, 64, 64], P('leaf'), may hold values from -0.75 to 0.75
- coupling: bfloat16 [1024, 1024], replicated, may hold values from -3 to 3, as said below
- parent: int32 [256], P('leaf'), may hold values from 0 to 15, never falling along the last dimension, each value on 1 to 24 neighbouring positions
- near_mask: int32 [256, 5], P('leaf'), may hold values from 0 to 1, as said below
- noise: float32 [131072], P('leaf'), may hold values from 0.5 to 2
- rhs: float32 [64, 131072], P('rep', 'leaf'), may hold values from -5 to 5
Outputs:
- solution: float32 [64, 131072], P('rep', 'leaf')
- residual: float32 [64, 131072], P('rep', 'leaf')
The draws below stay inside these ranges and needn't reach their ends.
Inputs may be any that keep to these rules, and one draw needn't show every extreme that they name: `coupling`: symmetric positive semidefinite. `parent`: never falling along the leaves. Slot 2 is 1; near_mask[l, 2 + o] = near_mask[l + o, 2 - o]; slots pointing before the first or after the last leaf are 0.
All inputs are finite; a program needn't handle non-finite values.
Results may differ from the reference program's by a relative error of at most 0.0003.
Values sent between devices are 32-bit elements; how exact they have to be, the bound alone decides.
No kernel may reach another device: no remote copies, remote signals or barrier semaphores. Data moves between devices by JAX's collectives and lax.ppermute only.
A program may use at most 64 MiB of HBM per device.

```python
import math
import jax
import jax.numpy as jnp
import numpy as np
from jax import lax

LEAF = 512
DIM = 8
RANK = 64
NRHS = 64
ITERS = 2
LEAF_DEV = 2
REACH = 2
LEAVES = 256
POINTS = 131072
LEVEL2 = 16
CHILD_MOST = 24


def leaf_centers(key):
    slopes = jax.random.uniform(jax.random.fold_in(key, 11), (DIM, 1), minval=0.1, maxval=0.25)
    phases = jax.random.uniform(jax.random.fold_in(key, 12), (DIM, 1), minval=-3.1, maxval=3.1)
    positions = jnp.arange(LEAVES, dtype=jnp.float32)[None, :]
    return 5.0 * jnp.sin(slopes * positions + phases)


def point_cloud(key):
    centers = leaf_centers(key)
    spread = jnp.clip(jax.random.normal(jax.random.fold_in(key, 13), (DIM, LEAVES, LEAF)), -3.0, 3.0)
    return (centers[:, :, None] + spread).reshape(DIM, LEAVES * LEAF)


def draw_coords(key, part):
    return point_cloud(key)


def draw_skeleton(key, part):
    centers = leaf_centers(key)
    spread = 0.8 * jnp.clip(jax.random.normal(jax.random.fold_in(key, 21), (DIM, LEAVES, RANK)), -3.0, 3.0)
    return (centers[:, :, None] + spread).reshape(DIM, LEAVES * RANK)


def draw_coupling(key, part):
    extent = LEVEL2 * RANK
    noise_part = jnp.clip(jax.random.normal(jax.random.fold_in(key, 31), (extent, extent)), -4.0, 4.0)
    factor = jnp.eye(extent, dtype=jnp.float32) + noise_part / jnp.sqrt(jnp.float32(extent))
    product = jnp.dot(factor, factor.T, precision=lax.Precision.HIGHEST)
    product = 0.5 * (product + product.T) / jnp.sqrt(jnp.float32(LEAVES // LEVEL2))
    return product.astype(jnp.bfloat16)


def draw_near_mask(key, part):
    crowded = jax.random.randint(jax.random.fold_in(key, 41), (LEAVES // LEAF_DEV,), 0, 4) == 0
    percent = jnp.repeat(jnp.where(crowded, 90, 15), LEAF_DEV)
    dice_rolls = jax.random.randint(jax.random.fold_in(key, 42), (LEAVES, REACH), 0, 100)
    leaf_index = jnp.arange(LEAVES, dtype=jnp.int32)[:, None]
    offsets = jnp.arange(1, REACH + 1, dtype=jnp.int32)[None, :]
    forward_pairs = (dice_rolls < percent[:, None]).astype(jnp.int32) * (leaf_index + offsets < LEAVES).astype(jnp.int32)
    behind = []
    for offset in range(REACH, 0, -1):
        moved = jnp.roll(forward_pairs[:, offset - 1], offset)
        behind.append(moved * (jnp.arange(LEAVES, dtype=jnp.int32) >= offset).astype(jnp.int32))
    middle = jnp.ones((LEAVES, 1), jnp.int32)
    return jnp.concatenate([jnp.stack(behind, axis=1), middle, forward_pairs], axis=1)


def draw_rhs(key, part):
    points = point_cloud(key)
    slopes = 0.15 * jax.random.normal(jax.random.fold_in(key, 51), (NRHS, DIM))
    phases = jax.random.uniform(jax.random.fold_in(key, 52), (NRHS, 1), minval=-3.1, maxval=3.1)
    smooth_wave = jnp.sin(jnp.dot(slopes, points, precision=lax.Precision.HIGHEST) + phases)
    rough_part = 0.3 * jnp.clip(jax.random.normal(jax.random.fold_in(key, 53), (NRHS, LEAVES * LEAF)), -3.0, 3.0)
    return smooth_wave + rough_part


def block_scale(key, shape, cuts, low, high):
    gain = 1.0
    for position, blocks in cuts:
        draws = jax.random.uniform(jax.random.fold_in(jax.random.fold_in(key, 6), position), (blocks,), jnp.float32, low / len(cuts), high / len(cuts))
        gain = gain * jnp.repeat(jnp.exp(draws), shape[position] // blocks).reshape((-1,) + (1,) * (len(shape) - 1 - position))
    return gain


def length_profile(number_of, total, bound, lean):
    portions = [(1 << 20) // math.isqrt(rank ** lean) + 1 for rank in range(2, number_of + 1)]
    spare, holding = total - bound - (number_of - 1), [1] * (number_of - 1)
    while spare > 0:
        free = [i for i in range(number_of - 1) if holding[i] < bound]
        mass, left = sum([portions[i] for i in free]), spare
        for i in free:
            addition = min(bound - holding[i], max(1, left * portions[i] // mass), spare)
            holding[i] = holding[i] + addition
            spare = spare - addition
    return np.array([bound] + holding)


def uneven(stream_key, count, total, limit, lean):
    if count == 2:
        one = jax.random.randint(stream_key, (), max(1, total - limit), min(limit, total - 1) + 1)
        return jnp.stack([one, total - one])
    tallies = jnp.asarray(length_profile(count, total, limit, lean), jnp.int32)
    pairs = (count - 1) // 2
    source_of, receiver = tallies[1:1 + 2 * pairs:2], tallies[2:2 + 2 * pairs:2]
    room = jnp.minimum(source_of - 1, limit - receiver)
    shifted = jax.random.randint(jax.random.fold_in(stream_key, 1), (pairs,), 0, 1 << 20) % (room + 1)
    tallies = tallies.at[1:1 + 2 * pairs:2].set(source_of - shifted).at[2:2 + 2 * pairs:2].set(receiver + shifted)
    return tallies[jax.random.permutation(jax.random.fold_in(stream_key, 2), count)]


def gaussian(stream_key, shape, deviation, reach, split=(), held_as=jnp.bfloat16):
    drawn = jax.random.normal(stream_key, shape, jnp.float32) * deviation
    if len(split) > 0:
        drawn = block_scale(stream_key, shape, split, -0.22, 0.18) * drawn
    return jnp.clip(drawn, min=-reach, max=reach).astype(held_as)


def setup_inputs(seed: int = 0) -> dict:
    key_of = jax.random.split(jax.random.key(seed), 9)
    coords = draw_coords(jax.random.fold_in(key_of[8], 71), 0)
    skeleton = draw_skeleton(jax.random.fold_in(key_of[8], 71), 0)
    transfer = gaussian(key_of[2], (LEAVES, RANK, RANK), RANK ** -0.5, 0.75, ((0, 128),))
    coupling = draw_coupling(jax.random.fold_in(key_of[8], 71), 0)
    parent = jnp.searchsorted(jnp.cumsum(uneven(key_of[4], LEVEL2, LEAVES, CHILD_MOST, 1)), jnp.arange(LEAVES), side="right").astype(jnp.int32)
    near_mask = draw_near_mask(jax.random.fold_in(key_of[8], 71), 0)
    noise = jnp.clip(jnp.exp(math.log(2.0) - 1.3862944 * jax.random.uniform(key_of[6], (POINTS,), jnp.float32) ** block_scale(key_of[6], (POINTS,), ((0, 128),), -0.2, 0.2)), 0.5, 2.0)
    rhs = draw_rhs(jax.random.fold_in(key_of[8], 71), 0)
    return {"coords": coords, "skeleton": skeleton, "transfer": transfer, "coupling": coupling, "parent": parent, "near_mask": near_mask, "noise": noise, "rhs": rhs}


HIGHEST = lax.Precision.HIGHEST
ROOT_THREE = 1.7320508075688772
LENGTH_SCALE = 4.0

def matern(row_coords, col_coords):
    cross = jnp.einsum('kdn,kdm->knm', row_coords, col_coords, precision=HIGHEST)
    first = lax.optimization_barrier(jnp.sum(row_coords * row_coords, axis=1))[:, :, None]
    second = lax.optimization_barrier(jnp.sum(col_coords * col_coords, axis=1))[:, None, :]
    scaled = ROOT_THREE / LENGTH_SCALE * jnp.sqrt(jnp.maximum(first + second - 2.0 * cross, 0.0))
    return (1.0 + scaled) * jnp.exp(-scaled)

def near_field(coords, values, near_mask):
    span_rows = REACH * LEAF
    col_width = (2 * REACH + 1) * LEAF
    padded_coords = jnp.pad(coords, ((0, 0), (span_rows, span_rows)))
    padded_values = jnp.pad(values, ((0, 0), (span_rows, span_rows)))

    def one_leaf(leaf_index):
        first_col = (leaf_index * LEAF).astype(jnp.int32)
        row_coords = lax.dynamic_slice_in_dim(coords, first_col, LEAF, 1)
        col_coords = lax.dynamic_slice_in_dim(padded_coords, first_col, col_width, 1)
        col_values = lax.dynamic_slice_in_dim(padded_values, first_col, col_width, 1)
        masking = jnp.repeat(near_mask[leaf_index].astype(jnp.float32), LEAF)
        kernel = matern(row_coords[None], col_coords[None])[0] * masking[None, :]
        return jnp.dot(col_values, kernel.T, precision=HIGHEST)
    blocks = lax.map(one_leaf, jnp.arange(LEAVES, dtype=jnp.int32))
    return jnp.transpose(blocks, (1, 0, 2)).reshape(NRHS, POINTS) / LEAF

def reference(coords, skeleton, transfer, coupling, parent, near_mask, noise, rhs):
    leaf_coords = jnp.transpose(coords.reshape(DIM, LEAVES, LEAF), (1, 0, 2))
    skeleton_coords = jnp.transpose(skeleton.reshape(DIM, LEAVES, RANK), (1, 0, 2))
    bases = matern(leaf_coords, skeleton_coords) / math.sqrt(LEAF)
    weights = transfer.astype(jnp.float32)
    coupled = coupling.astype(jnp.float32)
    members = (parent[:, None] == jnp.arange(LEVEL2, dtype=jnp.int32)[None, :]).astype(jnp.float32)
    counts = lax.optimization_barrier(jnp.sum(near_mask, axis=1)).astype(jnp.float32)
    diagonal = (noise.reshape(LEAVES, LEAF) + counts[:, None]).reshape(POINTS)

    def apply_operator(values):
        blocks = values.reshape(NRHS, LEAVES, LEAF)
        leaf_coeffs = jnp.einsum('cli,lir->lrc', blocks, bases, precision=HIGHEST)
        lifted = jnp.einsum('lrs,lrc->lsc', weights, leaf_coeffs, precision=HIGHEST)
        summed = jnp.einsum('lp,lsc->psc', members, lifted, precision=HIGHEST).reshape(LEVEL2 * RANK, NRHS)
        coupled_image = jnp.dot(coupled, summed, precision=HIGHEST)
        lowered = jnp.einsum('lp,psc->lsc', members, coupled_image.reshape(LEVEL2, RANK, NRHS), precision=HIGHEST)
        pushed = jnp.einsum('lrs,lsc->lrc', weights, lowered, precision=HIGHEST)
        far_part = jnp.einsum('lir,lrc->cli', bases, pushed, precision=HIGHEST).reshape(NRHS, POINTS)
        return diagonal[None, :] * values + near_field(coords, values, near_mask) + far_part
    solution = jnp.zeros_like(rhs)
    residual = rhs
    direction = rhs
    norm_now = lax.optimization_barrier(jnp.sum(residual * residual, axis=1))
    for iteration in range(ITERS):
        applied = apply_operator(direction)
        step_size = norm_now / lax.optimization_barrier(jnp.sum(direction * applied, axis=1))
        solution = solution + step_size[:, None] * direction
        residual = residual - step_size[:, None] * applied
        norm_next = lax.optimization_barrier(jnp.sum(residual * residual, axis=1))
        direction = residual + (norm_next / norm_now)[:, None] * direction
        norm_now = norm_next
    return (solution, residual)
```

```python
import functools
import math

import jax
import jax.numpy as jnp
from jax import lax
from jax.experimental import pallas as pl
from jax.experimental.pallas import tpu as pltpu
from jax.sharding import Mesh
from jax.sharding import PartitionSpec as P

LEAF = 512
DIM = 8
RANK = 64
LEVELS = 16
LEAVES_HERE = 2
SLOTS = 5
SPAN = LEAVES_HERE * LEAF
AXES = ("y", "z", "c")
HIGHEST = lax.Precision.HIGHEST
SCALE = math.sqrt(3.0) / 4.0
LOG2E = 1.4426950408889634
HALF = 256
F32 = jnp.float32
BF16 = jnp.bfloat16


def split(x, parts):
    out = []
    for _ in range(parts):
        piece = x.astype(BF16).astype(F32)
        out.append(piece)
        x = x - piece
    return out


def features(c):
    n = c.shape[1]
    c = c * SCALE
    p1, p2, p3 = split(c, 3)
    n1, n2, n3 = split(jnp.sum(c * c, axis=0, keepdims=True), 3)
    row = lax.broadcasted_iota(jnp.int32, (8, n), 0)
    def pick(*rows):
        out = jnp.zeros((8, n), F32)
        for at, value in rows:
            out = jnp.where(row == at, value, out)
        return out
    left_norm = pick((0, n1), (1, n2), (2, n3), (3, 1.0), (4, 1.0), (5, 1.0))
    right_norm = pick((0, 1.0), (1, 1.0), (2, 1.0), (3, n1), (4, n2), (5, n3))
    none = jnp.zeros((8, n), F32)
    q1, q2, q3 = -2.0 * p1, -2.0 * p2, -2.0 * p3
    left = jnp.concatenate([p1, p1, p2, p2, p1, p3, left_norm, none], axis=0)
    right = jnp.concatenate([q1, q2, q1, q2, q3, q1, right_norm, none], axis=0)
    return left, right


def matern(left, right):
    d2 = jnp.dot(left, right, preferred_element_type=F32)
    d2 = jnp.maximum(d2, 1e-30)
    s = d2 * lax.rsqrt(d2)
    return (1.0 + s) * jnp.exp2(s * -LOG2E)


def basis(own_right, skeleton, transfer, phi_ref):
    sk_left, _ = features(skeleton)
    for i in range(LEAVES_HERE):
        left = sk_left[:, RANK * i : RANK * (i + 1)].T.astype(BF16)
        bt = matern(left, own_right[i]) * (1.0 / math.sqrt(LEAF))
        phi_ref[i] = lax.dot_general(
            transfer[i].astype(F32), bt, (((0,), (0,)), ((), ())), precision=HIGHEST, preferred_element_type=F32
        )


def near_field(mask_ref, left_scr, right_scr, v_scr, acc_scr):
    acc_scr[...] = jnp.zeros(acc_scr.shape, F32)

    def block(b, carry):
        i = (b >= SLOTS).astype(jnp.int32)
        t = b - SLOTS * i

        @pl.when(mask_ref[i, t] > 0)
        def _():
            j = i + t
            right = right_scr[i]
            total = jnp.zeros((32, LEAF), F32)
            low = jnp.zeros((16, LEAF), F32)
            for h in range(LEAF // HALF):
                k = matern(left_scr[j, pl.ds(HALF * h, HALF), :], right)
                kh = k.astype(BF16)
                kl = (k - kh.astype(F32)).astype(BF16)
                v = v_scr[j, :, pl.ds(HALF * h, HALF)]
                total = total + jnp.dot(v, kh, preferred_element_type=F32)
                low = low + jnp.dot(v[:16], kl, preferred_element_type=F32)
            acc_scr[i] = acc_scr[i] + (total[:16] + total[16:] + low)

        return carry

    lax.fori_loop(0, LEAVES_HERE * SLOTS, block, 0)


def outgoing(parent_ref, v, local, phi_ref, send_ref):
    lane = lax.broadcasted_iota(jnp.int32, (16, 128), 1)
    norm = jnp.sum(v * v, axis=1, keepdims=True)
    inner = jnp.sum(v * local, axis=1, keepdims=True)
    base = jnp.where(lane == 64, norm, jnp.where(lane == 65, inner, 0.0))
    lifted = []
    for i in range(LEAVES_HERE):
        up = lax.dot_general(
            v[:, LEAF * i : LEAF * (i + 1)], phi_ref[i], (((1,), (1,)), ((), ())),
            precision=HIGHEST, preferred_element_type=F32,
        )
        lifted.append(jnp.concatenate([up, jnp.zeros((16, 64), F32)], axis=1))
    for p in range(LEVELS):
        w0 = (parent_ref[0] == p).astype(F32)
        w1 = (parent_ref[1] == p).astype(F32)
        send_ref[p] = base + w0 * lifted[0] + w1 * lifted[1]


def apply_kernel(mask_ref, parent_ref, coords_ref, lc_ref, rc_ref, skeleton_ref, transfer_ref, noise_ref,
                 v_ref, lv_ref, rv_ref, local_ref, phi_ref, send_ref, left_scr, right_scr, v_scr, acc_scr):
    for g, (c_ref, x_ref) in enumerate(((lc_ref, lv_ref), (coords_ref, v_ref), (rc_ref, rv_ref))):
        left, right = features(c_ref[...])
        for i in range(LEAVES_HERE):
            at = slice(LEAF * i, LEAF * (i + 1))
            left_scr[2 * g + i] = left[:, at].T.astype(BF16)
            if g == 1:
                right_scr[i] = right[:, at].astype(BF16)
            x = x_ref[:, LEAF * i : LEAF * (i + 1)] * (1.0 / LEAF)
            xh, xl = split(x, 2)
            v_scr[2 * g + i] = jnp.concatenate([xh, xl], axis=0).astype(BF16)
    basis([right_scr[i] for i in range(LEAVES_HERE)], skeleton_ref[...], transfer_ref[...], phi_ref)
    near_field(mask_ref, left_scr, right_scr, v_scr, acc_scr)
    v = v_ref[...]
    for i in range(LEAVES_HERE):
        count = mask_ref[i, 0]
        for t in range(1, SLOTS):
            count = count + mask_ref[i, t]
        at = slice(LEAF * i, LEAF * (i + 1))
        diagonal = noise_ref[:, at] + count.astype(F32)
        local_ref[:, at] = diagonal * v[:, at] + acc_scr[i]
    outgoing(parent_ref, v, local_ref[...], phi_ref, send_ref)


VMEM = pl.BlockSpec(memory_space=pltpu.VMEM)
SMEM = pl.BlockSpec(memory_space=pltpu.SMEM)


def apply_local(mask, parent, coords, lc, rc, skeleton, transfer, noise, v, lv, rv):
    return pl.pallas_call(
        apply_kernel,
        out_shape=(
            jax.ShapeDtypeStruct((16, SPAN), F32),
            jax.ShapeDtypeStruct((LEAVES_HERE, RANK, LEAF), F32),
            jax.ShapeDtypeStruct((LEVELS, 16, 128), F32),
        ),
        in_specs=[SMEM, SMEM] + [VMEM] * 9,
        out_specs=(VMEM, VMEM, VMEM),
        scratch_shapes=[
            pltpu.VMEM((6, LEAF, 64), BF16),
            pltpu.VMEM((2, 64, LEAF), BF16),
            pltpu.VMEM((6, 32, LEAF), BF16),
            pltpu.VMEM((2, 16, LEAF), F32),
        ],
        compiler_params=pltpu.CompilerParams(vmem_limit_bytes=24 * 1024 * 1024),
        name="apply_local",
    )(mask, parent, coords, lc, rc, skeleton, transfer, noise, v, lv, rv)


def far_field(parent_ref, got_ref, coupling_ref, phi_ref, img_scr):
    sums = jnp.concatenate([got_ref[p, :, :RANK] for p in range(LEVELS)], axis=1)
    parts = jnp.concatenate(split(sums, 3), axis=0).astype(BF16)
    image = jnp.dot(parts, coupling_ref[...], preferred_element_type=F32)
    image = image[:16] + image[16:32] + image[32:]
    scalars = got_ref[0]
    norm = scalars[:, 64:65]
    inner = scalars[:, 65:66] + jnp.sum(sums * image, axis=1, keepdims=True)
    for p in range(LEVELS):
        img_scr[p] = image[:, RANK * p : RANK * (p + 1)]
    far = []
    for i in range(LEAVES_HERE):
        far.append(jnp.dot(img_scr[parent_ref[i]], phi_ref[i], precision=HIGHEST, preferred_element_type=F32))
    return jnp.concatenate(far, axis=1), norm, inner


def first_kernel(parent_ref, got_ref, coupling_ref, phi_ref, local_ref, rhs_ref,
                 residual_ref, along_ref, kept_ref, img_scr):
    far, norm, inner = far_field(parent_ref, got_ref, coupling_ref, phi_ref, img_scr)
    along = local_ref[...] + far
    step = norm / inner
    residual_ref[...] = rhs_ref[...] - step * along
    along_ref[...] = along
    lane = lax.broadcasted_iota(jnp.int32, (16, 128), 1)
    kept_ref[...] = jnp.where(lane == 0, norm, jnp.where(lane == 1, step, 0.0))


def last_kernel(parent_ref, got_ref, coupling_ref, phi_ref, local_ref, rhs_ref, residual_ref, along_ref, kept_ref,
                solution_ref, out_ref, img_scr):
    far, norm, inner = far_field(parent_ref, got_ref, coupling_ref, phi_ref, img_scr)
    applied = local_ref[...] + far
    before = kept_ref[:, 0:1]
    first_step = kept_ref[:, 1:2]
    growth = norm / before
    step = norm / (inner - growth * norm / first_step)
    rhs = rhs_ref[...]
    residual = residual_ref[...]
    solution_ref[...] = first_step * rhs + step * (residual + growth * rhs)
    out_ref[...] = residual - step * (applied + growth * along_ref[...])


def first_update(parent, got, coupling, phi, local, rhs):
    return pl.pallas_call(
        first_kernel,
        out_shape=(
            jax.ShapeDtypeStruct((16, SPAN), F32),
            jax.ShapeDtypeStruct((16, SPAN), F32),
            jax.ShapeDtypeStruct((16, 128), F32),
        ),
        in_specs=[SMEM] + [VMEM] * 5,
        out_specs=(VMEM, VMEM, VMEM),
        scratch_shapes=[pltpu.VMEM((LEVELS, 16, RANK), F32)],
        compiler_params=pltpu.CompilerParams(vmem_limit_bytes=24 * 1024 * 1024),
        name="first_update",
    )(parent, got, coupling, phi, local, rhs)


def last_update(parent, got, coupling, phi, local, rhs, residual, along, kept):
    return pl.pallas_call(
        last_kernel,
        out_shape=(jax.ShapeDtypeStruct((16, SPAN), F32), jax.ShapeDtypeStruct((16, SPAN), F32)),
        in_specs=[SMEM] + [VMEM] * 8,
        out_specs=(VMEM, VMEM),
        scratch_shapes=[pltpu.VMEM((LEVELS, 16, RANK), F32)],
        compiler_params=pltpu.CompilerParams(vmem_limit_bytes=24 * 1024 * 1024),
        name="last_update",
    )(parent, got, coupling, phi, local, rhs, residual, along, kept)


def beside(x):
    count = lax.axis_size(AXES)
    left = lax.ppermute(x, AXES, [(i, i + 1) for i in range(count - 1)])
    right = lax.ppermute(x, AXES, [(i + 1, i) for i in range(count - 1)])
    return left, right


def total(send):
    mine = jnp.sum(lax.all_to_all(send, ("z", "c"), 0, 0, tiled=True), axis=0)
    rows = lax.axis_size("y")
    whole = jnp.sum(lax.all_to_all(jnp.broadcast_to(mine, (rows, *mine.shape)), "y", 0, 0, tiled=True), axis=0)
    return lax.all_to_all(jnp.broadcast_to(whole, send.shape), ("z", "c"), 0, 0, tiled=True)


def per_device(coords, skeleton, transfer, coupling, parent, near_mask, noise, rhs):
    lc, rc = beside(coords)
    lv, rv = beside(rhs)
    fixed = (skeleton, transfer, noise.reshape(1, SPAN))
    local, phi, send = apply_local(near_mask, parent, coords, lc, rc, *fixed, rhs, lv, rv)
    residual, along, kept = first_update(parent, total(send), coupling, phi, local, rhs)
    lv, rv = beside(residual)
    local, phi, send = apply_local(near_mask, parent, coords, lc, rc, *fixed, residual, lv, rv)
    return last_update(parent, total(send), coupling, phi, local, rhs, residual, along, kept)


def solution(mesh):
    finer = Mesh(mesh.devices.reshape(8, 8, 2, mesh.shape["rep"]), (*AXES, "rep"))
    placed = (
        P(None, AXES),
        P(None, AXES),
        P(AXES, None, None),
        P(),
        P(AXES),
        P(AXES, None),
        P(AXES),
        P("rep", AXES),
    )
    return jax.shard_map(
        per_device,
        mesh=finer,
        in_specs=placed,
        out_specs=(P("rep", AXES), P("rep", AXES)),
        check_vma=False,
    )
```

```python
import functools
import math

import jax
import jax.numpy as jnp
from jax import lax
from jax.experimental import pallas as pl
from jax.experimental.pallas import tpu as pltpu
from jax.sharding import Mesh
from jax.sharding import PartitionSpec as P

LEAF = 512
DIM = 8
RANK = 64
LEVELS = 16
LEAVES_HERE = 2
SLOTS = 5
SPAN = LEAVES_HERE * LEAF
AXES = ("y", "z", "c")
HIGHEST = lax.Precision.HIGHEST
SCALE = math.sqrt(3.0) / 4.0
LOG2E = 1.4426950408889634
HALF = 256
F32 = jnp.float32
BF16 = jnp.bfloat16


def split(x, parts):
    out = []
    for _ in range(parts):
        piece = x.astype(BF16).astype(F32)
        out.append(piece)
        x = x - piece
    return out


def features(c):
    n = c.shape[1]
    c = c * SCALE
    p1, p2, p3 = split(c, 3)
    n1, n2, n3 = split(jnp.sum(c * c, axis=0, keepdims=True), 3)
    row = lax.broadcasted_iota(jnp.int32, (8, n), 0)
    def pick(*rows):
        out = jnp.zeros((8, n), F32)
        for at, value in rows:
            out = jnp.where(row == at, value, out)
        return out
    left_norm = pick((0, n1), (1, n2), (2, n3), (3, 1.0), (4, 1.0), (5, 1.0))
    right_norm = pick((0, 1.0), (1, 1.0), (2, 1.0), (3, n1), (4, n2), (5, n3))
    none = jnp.zeros((8, n), F32)
    q1, q2, q3 = -2.0 * p1, -2.0 * p2, -2.0 * p3
    left = jnp.concatenate([p1, p1, p2, p2, p1, p3, left_norm, none], axis=0)
    right = jnp.concatenate([q1, q2, q1, q2, q3, q1, right_norm, none], axis=0)
    return left, right


def matern(left, right):
    d2 = jnp.dot(left, right, preferred_element_type=F32)
    d2 = jnp.maximum(d2, 1e-30)
    s = d2 * lax.rsqrt(d2)
    return (1.0 + s) * jnp.exp2(s * -LOG2E)


VMEM = pl.BlockSpec(memory_space=pltpu.VMEM)
SMEM = pl.BlockSpec(memory_space=pltpu.SMEM)
HBM = pl.BlockSpec(memory_space=pltpu.HBM)
LIMIT = 24 * 1024 * 1024
PAIRS = 4
ROWS_OUT = 24
ROWS_ACROSS = 16 * PAIRS + 8
TAIL = 80
BESIDE = 128 + TAIL


def off_chip(*arrays):
    return [pltpu.with_memory_space_constraint(x, pltpu.HBM) for x in arrays]


def shaped(*dims, dtype=F32):
    return jax.ShapeDtypeStruct(dims, dtype)


def call(kernel, name, in_specs, outs, scratch=(), kept=None):
    return pl.pallas_call(
        kernel,
        out_shape=tuple(outs),
        in_specs=in_specs,
        out_specs=tuple(HBM if n == kept else VMEM for n in range(len(outs))),
        scratch_shapes=list(scratch),
        compiler_params=pltpu.CompilerParams(vmem_limit_bytes=LIMIT),
        name=name,
    )


def leaf(i):
    return slice(LEAF * i, LEAF * (i + 1))


def halves(x):
    hi, lo = split(x * (1.0 / LEAF), 2)
    return jnp.concatenate([hi, lo], axis=0).astype(BF16)


def own_block(b):
    i = b // 2
    return i, 2 + b % 2


def halo_block(b):
    i = b // 3
    m = i + b % 3
    far = (m >= 2).astype(jnp.int32)
    return i, m + 2 * far


def active(mask_ref, place, b):
    i, j = place(b)
    return mask_ref[i, j - i] > 0


def evaluate(count, place, mask_ref, left_scr, right_scr, v_scr, k_scr, k_hbm, sems, acc_scr):
    def block(b, carry):
        i, j = place(b)

        @pl.when(active(mask_ref, place, b))
        def _():
            right = right_scr[i]
            total = jnp.zeros((32, LEAF), F32)
            low = jnp.zeros((16, LEAF), F32)
            for h in range(LEAF // HALF):
                rows = pl.ds(HALF * h, HALF)
                k = matern(left_scr[j, rows, :], right)
                kh = k.astype(BF16)
                kl = (k - kh.astype(F32)).astype(BF16)
                k_scr[b, 0, rows, :] = kh
                k_scr[b, 1, rows, :] = kl
                v = v_scr[j, :, rows]
                total = total + jnp.dot(v, kh, preferred_element_type=F32)
                low = low + jnp.dot(v[:16], kl, preferred_element_type=F32)
            pltpu.make_async_copy(k_scr.at[b], k_hbm.at[b], sems.at[b]).start()
            acc_scr[i] = acc_scr[i] + (total[:16] + total[16:] + low)

        return carry

    lax.fori_loop(0, count, block, 0)


def each_active(count, place, mask_ref, action):
    for b in range(count):
        pl.when(active(mask_ref, place, jnp.int32(b)))(functools.partial(action, b))


def sent(count, place, mask_ref, k_scr, k_hbm, sems):
    each_active(count, place, mask_ref, lambda b: pltpu.make_async_copy(k_scr.at[b], k_hbm.at[b], sems.at[b]).wait())


def fetched(count, place, mask_ref, k_hbm, k_scr, sems):
    each_active(count, place, mask_ref, lambda b: pltpu.make_async_copy(k_hbm.at[b], k_scr.at[b], sems.at[b]).start())


def apply_kept(count, place, mask_ref, v_scr, k_scr, k_hbm, sems, acc_scr):
    def block(b, carry):
        i, j = place(b)

        @pl.when(active(mask_ref, place, b))
        def _():
            pltpu.make_async_copy(k_hbm.at[b], k_scr.at[b], sems.at[b]).wait()
            v = v_scr[j]
            total = jnp.dot(v, k_scr[b, 0], preferred_element_type=F32)
            low = jnp.dot(v[:16], k_scr[b, 1], preferred_element_type=F32)
            acc_scr[i] = acc_scr[i] + (total[:16] + total[16:] + low)

        return carry

    lax.fori_loop(0, count, block, 0)


def lifted(v, phi_ref):
    up = [
        lax.dot_general(
            v[:, leaf(i)], phi_ref[i], (((1,), (1,)), ((), ())), precision=HIGHEST, preferred_element_type=F32
        )
        for i in range(LEAVES_HERE)
    ]
    return jnp.concatenate(up, axis=1)


def post(parent_ref, up, v, local, send_ref):
    lane = lax.broadcasted_iota(jnp.int32, (8, 128), 1)
    norm = jnp.sum(v * v, axis=1, keepdims=True)
    inner = jnp.sum(v * local, axis=1, keepdims=True)
    tile = jnp.zeros((8, 128), F32)
    for at, value in enumerate(
        (norm[:8], inner[:8], norm[8:], inner[8:], parent_ref[0].astype(F32), parent_ref[1].astype(F32))
    ):
        tile = jnp.where(lane == at, value, tile)
    for d in range(send_ref.shape[0]):
        send_ref[d, :16, :] = up
        send_ref[d, 16:, :] = tile


def paired(tiles):
    lane = lax.broadcasted_iota(jnp.int32, (16, 128), 1)
    whole = [t + pltpu.roll(t, 64, axis=1) for t in tiles]
    return [jnp.where(lane < 64, whole[m], whole[m + 1]) for m in range(0, len(tiles), 2)]


def across_kernel(got_ref, send_ref):
    lane = lax.broadcasted_iota(jnp.int32, (1, 128), 1)
    first = got_ref[0, 16:17, 4:5]
    tiles = [jnp.zeros((16, 128), F32) for _ in range(2 * PAIRS)]
    scalars = jnp.zeros((8, 128), F32)
    for d in range(got_ref.shape[0]):
        slot = jnp.where(lane < 64, got_ref[d, 16:17, 4:5], got_ref[d, 16:17, 5:6]) - first
        piece = got_ref[d, :16, :]
        for s in range(2 * PAIRS):
            tiles[s] = tiles[s] + jnp.where(slot == float(s), piece, 0.0)
        scalars = scalars + got_ref[d, 16:, :]
    scalars = jnp.where(lane == 4, first, scalars)
    tiles = paired(tiles)
    for y in range(send_ref.shape[0]):
        for k in range(PAIRS):
            send_ref[y, 16 * k : 16 * (k + 1), :] = tiles[k]
        send_ref[y, 16 * PAIRS :, :] = scalars


def whole_sums(got_ref):
    lane = lax.broadcasted_iota(jnp.int32, (1, 128), 1)
    half = (lane >= 64).astype(F32)
    tiles = [jnp.zeros((16, 128), F32) for _ in range(LEVELS)]
    scalars = jnp.zeros((8, 128), F32)
    for y in range(got_ref.shape[0]):
        first = got_ref[y, 16 * PAIRS : 16 * PAIRS + 1, 4:5] + half
        for k in range(PAIRS):
            piece = got_ref[y, 16 * k : 16 * (k + 1), :]
            cluster = first + float(2 * k)
            for q in range(LEVELS):
                tiles[q] = tiles[q] + jnp.where(cluster == float(q), piece, 0.0)
        scalars = scalars + got_ref[y, 16 * PAIRS :, :]
    norm = jnp.concatenate([scalars[:, 0:1], scalars[:, 2:3]], axis=0)
    inner = jnp.concatenate([scalars[:, 1:2], scalars[:, 3:4]], axis=0)
    return jnp.concatenate(paired(tiles), axis=1), norm, inner


def coupled_image(got_ref, coupling_hbm, coupling_ref, sem, img_scr, also=lambda: None):
    fetch = pltpu.make_async_copy(coupling_hbm, coupling_ref, sem)
    fetch.start()
    also()
    sums, norm, inner = whole_sums(got_ref)
    parts = jnp.concatenate(split(sums, 3), axis=0).astype(BF16)
    fetch.wait()
    image = jnp.dot(parts, coupling_ref[...], preferred_element_type=F32)
    image = image[:16] + image[16:32] + image[32:]
    inner = inner + jnp.sum(sums * image, axis=1, keepdims=True)
    for p in range(LEVELS):
        img_scr[p] = image[:, RANK * p : RANK * (p + 1)]
    return norm, inner


def own_far(parent_ref, phi_ref, img_scr):
    far = [
        jnp.dot(img_scr[parent_ref[i]], phi_ref[i], precision=HIGHEST, preferred_element_type=F32)
        for i in range(LEAVES_HERE)
    ]
    return jnp.concatenate(far, axis=1)


def prepare_kernel(parent_ref, mask_ref, coords_hbm, skeleton_hbm, transfer_hbm, noise_hbm, rhs_hbm,
                   right_ref, phi_ref, k_hbm, part_ref, up_ref, diag_ref, rhs_ref, tail_ref,
                   coords_scr, skeleton_scr, transfer_scr, noise_scr, left_scr, v_scr, acc_scr, k_scr, k_sems, sems):
    copies = [
        pltpu.make_async_copy(src, dst, sems.at[n])
        for n, (src, dst) in enumerate((
            (coords_hbm, coords_scr), (skeleton_hbm, skeleton_scr), (transfer_hbm, transfer_scr),
            (rhs_hbm, rhs_ref), (noise_hbm, noise_scr),
        ))
    ]
    for copy in copies:
        copy.start()
    copies[0].wait()
    left, right = features(coords_scr[...])
    for i in range(LEAVES_HERE):
        left_scr[2 + i] = left[:, leaf(i)].T.astype(BF16)
        right_ref[i] = right[:, leaf(i)].astype(BF16)
    copies[1].wait()
    copies[2].wait()
    skeleton = skeleton_scr[...]
    sk_left, _ = features(skeleton)
    moved = [transfer_scr[i].astype(F32) for i in range(LEAVES_HERE)]
    for i in range(LEAVES_HERE):
        rows = sk_left[:, RANK * i : RANK * (i + 1)].T.astype(BF16)
        bt = matern(rows, right_ref[i]) * (1.0 / math.sqrt(LEAF))
        phi_ref[i] = lax.dot_general(
            moved[i], bt, (((0,), (0,)), ((), ())), precision=HIGHEST, preferred_element_type=F32
        )
    tail_ref[:64, :] = jnp.concatenate(moved, axis=1)
    tail_ref[64:72, :] = skeleton
    lane = lax.broadcasted_iota(jnp.int32, (8, 128), 1)
    tail_ref[72:, :] = jnp.where(lane < 64, parent_ref[0].astype(F32), parent_ref[1].astype(F32))
    copies[3].wait()
    v = rhs_ref[...]
    for i in range(LEAVES_HERE):
        v_scr[2 + i] = halves(v[:, leaf(i)])
    acc_scr[...] = jnp.zeros(acc_scr.shape, F32)
    evaluate(4, own_block, mask_ref, left_scr, right_ref, v_scr, k_scr, k_hbm, k_sems, acc_scr)
    up_ref[...] = lifted(v, phi_ref)
    copies[4].wait()
    for i in range(LEAVES_HERE):
        count = mask_ref[i, 0]
        for t in range(1, SLOTS):
            count = count + mask_ref[i, t]
        diag_ref[:, leaf(i)] = noise_scr[:, leaf(i)] + count.astype(F32)
        part_ref[:, leaf(i)] = diag_ref[:, leaf(i)] * v[:, leaf(i)] + acc_scr[i]
    sent(4, own_block, mask_ref, k_scr, k_hbm, k_sems)


def prepare(parent, mask, coords, skeleton, transfer, noise, rhs):
    return call(
        prepare_kernel, "prepare", [SMEM, SMEM] + [HBM] * 5,
        (
            shaped(2, 64, LEAF, dtype=BF16), shaped(2, RANK, LEAF), pltpu.HBM((4, 2, LEAF, LEAF), BF16),
            shaped(16, SPAN), shaped(16, 128), shaped(1, SPAN), shaped(16, SPAN), shaped(TAIL, 128),
        ),
        (
            pltpu.VMEM((DIM, SPAN), F32), pltpu.VMEM((DIM, 128), F32), pltpu.VMEM((2, RANK, RANK), BF16),
            pltpu.VMEM((1, SPAN), F32), pltpu.VMEM((4, LEAF, 64), BF16), pltpu.VMEM((4, 32, LEAF), BF16),
            pltpu.VMEM((2, 16, LEAF), F32), pltpu.VMEM((4, 2, LEAF, LEAF), BF16), pltpu.SemaphoreType.DMA((4,)),
            pltpu.SemaphoreType.DMA((5,)),
        ),
        kept=2,
    )(parent, mask, *off_chip(coords, skeleton, transfer, noise, rhs))


def first_kernel(parent_ref, mask_ref, before_ref, after_ref, right_ref, part_ref, up_ref, rhs_ref, tail_ref,
                 k_hbm, halo_right_ref, local_ref, beside_ref, send_ref, left_scr, v_scr, acc_scr, k_scr, k_sems):
    for g, ref in enumerate((before_ref, after_ref)):
        left, right = features(ref[:DIM, :])
        for i in range(LEAVES_HERE):
            left_scr[4 * g + i] = left[:, leaf(i)].T.astype(BF16)
            halo_right_ref[2 * g + i] = right[:, leaf(i)].astype(BF16)
            v_scr[4 * g + i] = halves(ref[DIM:, leaf(i)])
    for i in range(LEAVES_HERE):
        acc_scr[i] = part_ref[:, leaf(i)]
    evaluate(6, halo_block, mask_ref, left_scr, right_ref, v_scr, k_scr, k_hbm, k_sems, acc_scr)
    local = jnp.concatenate([acc_scr[i] for i in range(LEAVES_HERE)], axis=1)
    local_ref[...] = local
    for n in range(SPAN // 128):
        beside_ref[16 * n : 16 * (n + 1), :] = local[:, 128 * n : 128 * (n + 1)]
    beside_ref[128:, :] = tail_ref[...]
    post(parent_ref, up_ref[...], rhs_ref[...], local, send_ref)
    sent(6, halo_block, mask_ref, k_scr, k_hbm, k_sems)


def first(parent, mask, before, after, right, part, up, rhs, tail, peers):
    return call(
        first_kernel, "first", [SMEM, SMEM] + [VMEM] * 7,
        (
            pltpu.HBM((6, 2, LEAF, LEAF), BF16), shaped(4, 64, LEAF, dtype=BF16),
            shaped(16, SPAN), shaped(BESIDE, 128), shaped(peers, ROWS_OUT, 128),
        ),
        (
            pltpu.VMEM((6, LEAF, 64), BF16), pltpu.VMEM((6, 32, LEAF), BF16), pltpu.VMEM((2, 16, LEAF), F32),
            pltpu.VMEM((6, 2, LEAF, LEAF), BF16), pltpu.SemaphoreType.DMA((6,)),
        ),
        kept=0,
    )(parent, mask, before, after, right, part, up, rhs, tail)


def across(got, rows):
    return call(across_kernel, "across", [VMEM], (shaped(rows, ROWS_ACROSS, 128),))(got)[0]


def second_kernel(parent_ref, mask_ref, coupling_hbm, own_hbm, halo_hbm, got_ref, phi_ref, local_ref, rhs_ref,
                  diag_ref, before_ref, after_ref, halo_before_ref, halo_after_ref, halo_right_ref,
                  residual_ref, along_ref, kept_ref, out_ref, send_ref, img_scr, v_scr, acc_scr,
                  coupling_scr, own_scr, halo_scr, sem, own_sems, halo_sems):
    norm, inner = coupled_image(
        got_ref, coupling_hbm, coupling_scr, sem, img_scr,
        lambda: (
            fetched(4, own_block, mask_ref, own_hbm, own_scr, own_sems),
            fetched(6, halo_block, mask_ref, halo_hbm, halo_scr, halo_sems),
        ),
    )
    step = norm / inner
    along = local_ref[...] + own_far(parent_ref, phi_ref, img_scr)
    residual = rhs_ref[...] - step * along
    along_ref[...] = along
    residual_ref[...] = residual
    lane = lax.broadcasted_iota(jnp.int32, (16, 128), 1)
    kept_ref[...] = jnp.where(lane == 0, norm, jnp.where(lane == 1, step, 0.0))
    for i in range(LEAVES_HERE):
        v_scr[2 + i] = halves(residual[:, leaf(i)])
    for g, (msg_ref, ref) in enumerate(((halo_before_ref, before_ref), (halo_after_ref, after_ref))):
        sk_left, _ = features(msg_ref[192:200, :])
        for i in range(LEAVES_HERE):
            rows = sk_left[:, RANK * i : RANK * (i + 1)].T.astype(BF16)
            bt = matern(rows, halo_right_ref[2 * g + i]) * (1.0 / math.sqrt(LEAF))
            parent = jnp.max(msg_ref[200:208, RANK * i : RANK * (i + 1)]).astype(jnp.int32)
            image = img_scr[parent]
            pushed = lax.dot_general(
                image, msg_ref[128:192, RANK * i : RANK * (i + 1)], (((1,), (1,)), ((), ())),
                precision=HIGHEST, preferred_element_type=F32,
            )
            far = jnp.dot(pushed, bt, precision=HIGHEST, preferred_element_type=F32)
            local = jnp.concatenate([msg_ref[16 * n : 16 * (n + 1), :] for n in range(4 * i, 4 * (i + 1))], axis=1)
            v_scr[4 * g + i] = halves(ref[DIM:, leaf(i)] - step * (local + far))
    acc_scr[...] = jnp.zeros(acc_scr.shape, F32)
    apply_kept(4, own_block, mask_ref, v_scr, own_scr, own_hbm, own_sems, acc_scr)
    apply_kept(6, halo_block, mask_ref, v_scr, halo_scr, halo_hbm, halo_sems, acc_scr)
    near = jnp.concatenate([acc_scr[i] for i in range(LEAVES_HERE)], axis=1)
    local = diag_ref[...] * residual + near
    out_ref[...] = local
    post(parent_ref, lifted(residual, phi_ref), residual, local, send_ref)


COUPLING = pltpu.VMEM((LEVELS * RANK, LEVELS * RANK), BF16)


def second(parent, mask, coupling, own, halo, *arrays, peers):
    return call(
        second_kernel, "second", [SMEM, SMEM] + [HBM] * 3 + [VMEM] * len(arrays),
        (
            shaped(16, SPAN), shaped(16, SPAN), shaped(16, 128), shaped(16, SPAN), shaped(peers, ROWS_OUT, 128),
        ),
        (
            pltpu.VMEM((LEVELS, 16, RANK), F32), pltpu.VMEM((6, 32, LEAF), BF16), pltpu.VMEM((2, 16, LEAF), F32),
            COUPLING, pltpu.VMEM((4, 2, LEAF, LEAF), BF16), pltpu.VMEM((6, 2, LEAF, LEAF), BF16),
            pltpu.SemaphoreType.DMA, pltpu.SemaphoreType.DMA((4,)), pltpu.SemaphoreType.DMA((6,)),
        ),
    )(parent, mask, *off_chip(coupling, own, halo), *arrays)


def last_kernel(parent_ref, coupling_hbm, got_ref, phi_ref, local_ref, rhs_ref, residual_ref, along_ref, kept_ref,
                solution_ref, out_ref, img_scr, coupling_scr, sem):
    norm, inner = coupled_image(got_ref, coupling_hbm, coupling_scr, sem, img_scr)
    applied = local_ref[...] + own_far(parent_ref, phi_ref, img_scr)
    before = kept_ref[:, 0:1]
    first_step = kept_ref[:, 1:2]
    growth = norm / before
    step = norm / (inner - growth * norm / first_step)
    rhs = rhs_ref[...]
    residual = residual_ref[...]
    solution_ref[...] = first_step * rhs + step * (residual + growth * rhs)
    out_ref[...] = residual - step * (applied + growth * along_ref[...])


def last(parent, coupling, *arrays):
    return call(
        last_kernel, "last", [SMEM, HBM] + [VMEM] * len(arrays), (shaped(16, SPAN), shaped(16, SPAN)),
        (pltpu.VMEM((LEVELS, 16, RANK), F32), COUPLING, pltpu.SemaphoreType.DMA),
    )(parent, *off_chip(coupling), *arrays)


def beside(x):
    count = lax.axis_size(AXES)
    before = lax.ppermute(x, AXES, [(i, i + 1) for i in range(count - 1)])
    after = lax.ppermute(x, AXES, [(i + 1, i) for i in range(count - 1)])
    return before, after


def exchange(send):
    row = lax.all_to_all(send, ("z", "c"), 0, 0, tiled=True)
    return lax.all_to_all(across(row, lax.axis_size("y")), "y", 0, 0, tiled=True)


def per_device(coords, skeleton, transfer, coupling, parent, near_mask, noise, rhs):
    peers = lax.axis_size(("z", "c"))
    before, after = beside(jnp.concatenate([coords, rhs], axis=0))
    right, phi, k_own, part, up, diag, rhs, tail = prepare(
        parent, near_mask, coords, skeleton, transfer, noise.reshape(1, SPAN), rhs
    )
    k_halo, halo_right, local, message, send = first(
        parent, near_mask, before, after, right, part, up, rhs, tail, peers
    )
    halo_before, halo_after = beside(message)
    residual, along, kept, local, send = second(
        parent, near_mask, coupling, k_own, k_halo, exchange(send), phi, local, rhs, diag,
        before, after, halo_before, halo_after, halo_right, peers=peers,
    )
    return last(parent, coupling, exchange(send), phi, local, rhs, residual, along, kept)


def solution(mesh):
    finer = Mesh(mesh.devices.reshape(8, 8, 2, mesh.shape["rep"]), (*AXES, "rep"))
    placed = (
        P(None, AXES),
        P(None, AXES),
        P(AXES, None, None),
        P(),
        P(AXES),
        P(AXES, None),
        P(AXES),
        P("rep", AXES),
    )
    return jax.shard_map(
        per_device,
        mesh=finer,
        in_specs=placed,
        out_specs=(P("rep", AXES), P("rep", AXES)),
        check_vma=False,
    )
```

```python
import math

import jax
import jax.numpy as jnp
from jax import lax
from jax.experimental import pallas as pl
from jax.experimental.pallas import tpu as pltpu
from jax.sharding import Mesh
from jax.sharding import PartitionSpec as P


LEAF = 512
DIM = 8
RANK = 64
LEVELS = 16
LEAVES_HERE = 2
SLOTS = 5
SPAN = LEAVES_HERE * LEAF
AXES = ("y", "z", "c")
SCALE = math.sqrt(3.0) / 4.0
LOG2E = 1.4426950408889634
CHUNK = 64
SLOTS_KEPT = 2
F32 = jnp.float32
BF16 = jnp.bfloat16


def split(x, parts):
    out = []
    for _ in range(parts):
        piece = x.astype(BF16).astype(F32)
        out.append(piece)
        x = x - piece
    return out


def pair(x):
    hi, lo = split(x, 2)
    return hi.astype(BF16), lo.astype(BF16)


def pair_dot(x, hi, lo, contract=0):
    dims = (((1,), (contract,)), ((), ()))
    xh, xl = split(x, 2)
    both = jnp.concatenate([xh, xl], axis=0).astype(BF16)
    wide = lax.dot_general(both, hi, dims, preferred_element_type=F32)
    low = lax.dot_general(xh.astype(BF16), lo, dims, preferred_element_type=F32)
    return wide[:16] + wide[16:] + low


def features(c):
    n = c.shape[1]
    c = c * SCALE
    p1, p2, p3 = split(c, 3)
    n1, n2, n3 = split(jnp.sum(c * c, axis=0, keepdims=True), 3)
    row = lax.broadcasted_iota(jnp.int32, (8, n), 0)
    def pick(*rows):
        out = jnp.zeros((8, n), F32)
        for at, value in rows:
            out = jnp.where(row == at, value, out)
        return out
    left_norm = pick((0, n1), (1, n2), (2, n3), (3, 1.0), (4, 1.0), (5, 1.0))
    right_norm = pick((0, 1.0), (1, 1.0), (2, 1.0), (3, n1), (4, n2), (5, n3))
    none = jnp.zeros((8, n), F32)
    q1, q2, q3 = -2.0 * p1, -2.0 * p2, -2.0 * p3
    left = jnp.concatenate([p1, p1, p2, p2, p1, p3, left_norm, none], axis=0)
    right = jnp.concatenate([q1, q2, q1, q2, q3, q1, right_norm, none], axis=0)
    return left, right


def matern(left, right):
    d2 = jnp.dot(left, right, preferred_element_type=F32)
    d2 = jnp.maximum(d2, 1e-30)
    s = d2 * lax.rsqrt(d2)
    return (1.0 + s) * jnp.exp2(s * -LOG2E)


VMEM = pl.BlockSpec(memory_space=pltpu.VMEM)
SMEM = pl.BlockSpec(memory_space=pltpu.SMEM)
HBM = pl.BlockSpec(memory_space=pltpu.HBM)
LIMIT = 24 * 1024 * 1024
PAIRS = 4
ROWS_OUT = 24
ROWS_ACROSS = 16 * PAIRS + 8
TAIL = 80
BESIDE = 128 + TAIL


def off_chip(*arrays):
    return [pltpu.with_memory_space_constraint(x, pltpu.HBM) for x in arrays]


def shaped(*dims, dtype=F32):
    return jax.ShapeDtypeStruct(dims, dtype)


def call(kernel, in_specs, outs, scratch=()):
    return pl.pallas_call(
        kernel,
        out_shape=tuple(outs),
        in_specs=in_specs,
        out_specs=tuple(VMEM for _ in outs),
        scratch_shapes=list(scratch),
        compiler_params=pltpu.CompilerParams(vmem_limit_bytes=LIMIT),
    )


def leaf(i):
    return slice(LEAF * i, LEAF * (i + 1))


def halves(x):
    hi, lo = split(x * (1.0 / LEAF), 2)
    return jnp.concatenate([hi, lo], axis=0).astype(BF16)


def own_block(b):
    i = b // 2
    return i, 2 + b % 2


def halo_at(j):
    return j - 2 * ((j >= 4) * 1)


def halo_block(b):
    i = b // 3
    m = i + b % 3
    far = (m >= 2) * 1
    return i, m + 2 * far


def near_field(count, place, mask_ref, left_of, right_of, v_scr, acc_scr, k_scr):
    for b in range(count):
        i, j = place(b)
        slot = b % SLOTS_KEPT
        right = right_of(i)
        for h in range(LEAF // CHUNK):
            rows = slice(CHUNK * h, CHUNK * (h + 1))
            k = matern(left_of(j, rows), right)
            kh = k.astype(BF16)
            k_scr[slot, 0, rows, :] = kh
            k_scr[slot, 1, rows, :] = (k - kh.astype(F32)).astype(BF16)
        v = v_scr[j]
        total = jnp.dot(v, k_scr[slot, 0], preferred_element_type=F32)
        low = jnp.dot(v[:16], k_scr[slot, 1], preferred_element_type=F32)
        acc_scr[i] = acc_scr[i] + mask_ref[i, j - i].astype(F32) * (total[:16] + total[16:] + low)


def fetch(pairs, sems):
    copies = [pltpu.make_async_copy(src, dst, sems.at[n]) for n, (src, dst) in enumerate(pairs)]
    for copy in copies:
        copy.start()
    return copies


def lifted(v, phi_ref):
    return jnp.concatenate(
        [pair_dot(v[:, leaf(i)], phi_ref[i, 0], phi_ref[i, 1], contract=1) for i in range(LEAVES_HERE)], axis=1
    )


def post(parent_ref, up, v, local, send_ref):
    lane = lax.broadcasted_iota(jnp.int32, (8, 128), 1)
    norm = jnp.sum(v * v, axis=1, keepdims=True)
    inner = jnp.sum(v * local, axis=1, keepdims=True)
    tile = jnp.zeros((8, 128), F32)
    for at, value in enumerate(
        (norm[:8], inner[:8], norm[8:], inner[8:], parent_ref[0].astype(F32), parent_ref[1].astype(F32))
    ):
        tile = jnp.where(lane == at, value, tile)
    for d in range(send_ref.shape[0]):
        send_ref[d, :16, :] = up
        send_ref[d, 16:, :] = tile


def paired(tiles):
    lane = lax.broadcasted_iota(jnp.int32, (16, 128), 1)
    whole = [t + pltpu.roll(t, 64, axis=1) for t in tiles]
    return [jnp.where(lane < 64, whole[m], whole[m + 1]) for m in range(0, len(tiles), 2)]


def across_kernel(got_ref, send_ref):
    lane = lax.broadcasted_iota(jnp.int32, (1, 128), 1)
    first = got_ref[0, 16:17, 4:5]
    tiles = [jnp.zeros((16, 128), F32) for _ in range(2 * PAIRS)]
    scalars = jnp.zeros((8, 128), F32)
    for d in range(got_ref.shape[0]):
        slot = jnp.where(lane < 64, got_ref[d, 16:17, 4:5], got_ref[d, 16:17, 5:6]) - first
        piece = got_ref[d, :16, :]
        for s in range(2 * PAIRS):
            tiles[s] = tiles[s] + jnp.where(slot == float(s), piece, 0.0)
        scalars = scalars + got_ref[d, 16:, :]
    scalars = jnp.where(lane == 4, first, scalars)
    tiles = paired(tiles)
    for y in range(send_ref.shape[0]):
        for k in range(PAIRS):
            send_ref[y, 16 * k : 16 * (k + 1), :] = tiles[k]
        send_ref[y, 16 * PAIRS :, :] = scalars


def whole_sums(got_ref):
    lane = lax.broadcasted_iota(jnp.int32, (1, 128), 1)
    half = (lane >= 64).astype(F32)
    tiles = [jnp.zeros((16, 128), F32) for _ in range(LEVELS)]
    scalars = jnp.zeros((8, 128), F32)
    for y in range(got_ref.shape[0]):
        first = got_ref[y, 16 * PAIRS : 16 * PAIRS + 1, 4:5] + half
        for k in range(PAIRS):
            piece = got_ref[y, 16 * k : 16 * (k + 1), :]
            cluster = first + float(2 * k)
            for q in range(LEVELS):
                tiles[q] = tiles[q] + jnp.where(cluster == float(q), piece, 0.0)
        scalars = scalars + got_ref[y, 16 * PAIRS :, :]
    norm = jnp.concatenate([scalars[:, 0:1], scalars[:, 2:3]], axis=0)
    inner = jnp.concatenate([scalars[:, 1:2], scalars[:, 3:4]], axis=0)
    return jnp.concatenate(paired(tiles), axis=1), norm, inner


def coupled_image(got_ref, coupling_ref, img_scr, ready=lambda: None):
    sums, norm, inner = whole_sums(got_ref)
    parts = jnp.concatenate(split(sums, 3), axis=0).astype(BF16)
    ready()
    image = jnp.dot(parts, coupling_ref[...], preferred_element_type=F32)
    image = image[:16] + image[16:32] + image[32:]
    inner = inner + jnp.sum(sums * image, axis=1, keepdims=True)
    for p in range(LEVELS):
        img_scr[p] = image[:, RANK * p : RANK * (p + 1)]
    return norm, inner


def own_far(parent_ref, phi_ref, img_scr):
    return jnp.concatenate(
        [pair_dot(img_scr[parent_ref[i]], phi_ref[i, 0], phi_ref[i, 1]) for i in range(LEAVES_HERE)], axis=1
    )


def pack_kernel(coords_hbm, skeleton_hbm, transfer_hbm, noise_hbm, rhs_hbm, packed_ref, skeleton_ref, transfer_ref,
                noise_ref, sems):
    for copy in fetch(
        (
            (rhs_hbm, packed_ref.at[pl.ds(DIM, 16), :]), (coords_hbm, packed_ref.at[pl.ds(0, DIM), :]),
            (transfer_hbm, transfer_ref), (skeleton_hbm, skeleton_ref), (noise_hbm, noise_ref),
        ),
        sems,
    ):
        copy.wait()


def pack(coords, skeleton, transfer, noise, rhs):
    return call(
        pack_kernel, [HBM] * 5,
        (shaped(24, SPAN), shaped(DIM, 128), shaped(2, RANK, RANK, dtype=BF16), shaped(1, SPAN)),
        (pltpu.SemaphoreType.DMA((5,)),),
    )(*off_chip(coords, skeleton, transfer, noise, rhs))


FLAGS = [pltpu.SMEM((2,), jnp.int32), pltpu.SMEM((2, SLOTS), jnp.int32)]


def prepare_kernel(parent_hbm, mask_hbm, packed_ref, skeleton_ref, transfer_ref, noise_ref,
                   left_ref, right_ref, phi_ref, part_ref, up_ref, diag_ref, tail_ref,
                   parent_ref, mask_ref, v_scr, acc_scr, k_scr, sems):
    flags = fetch(((parent_hbm, parent_ref), (mask_hbm, mask_ref)), sems)
    left, right = features(packed_ref[:DIM, :])
    v = packed_ref[DIM:, :]
    for i in range(LEAVES_HERE):
        left_ref[i] = left[:, leaf(i)].T.astype(BF16)
        right_ref[i] = right[:, leaf(i)].astype(BF16)
        v_scr[2 + i] = halves(v[:, leaf(i)])
    skeleton = skeleton_ref[...]
    sk_left, _ = features(skeleton)
    for i in range(LEAVES_HERE):
        rows = sk_left[:, RANK * i : RANK * (i + 1)].T.astype(BF16)
        bt = matern(rows, right_ref[i]) * (1.0 / math.sqrt(LEAF))
        moved = transfer_ref[i]
        phi = jnp.zeros((RANK, LEAF), F32)
        for part in split(bt, 3):
            phi = phi + lax.dot_general(
                moved, part.astype(BF16), (((0,), (0,)), ((), ())), preferred_element_type=F32
            )
        phi_ref[i, 0], phi_ref[i, 1] = pair(phi)
    tail_ref[:64, :] = jnp.concatenate([transfer_ref[i].astype(F32) for i in range(LEAVES_HERE)], axis=1)
    tail_ref[64:72, :] = skeleton
    up_ref[...] = lifted(v, phi_ref)
    acc_scr[...] = jnp.zeros(acc_scr.shape, F32)
    for flag in flags:
        flag.wait()
    lane = lax.broadcasted_iota(jnp.int32, (8, 128), 1)
    tail_ref[72:, :] = jnp.where(lane < 64, parent_ref[0].astype(F32), parent_ref[1].astype(F32))
    near_field(4, own_block, mask_ref, lambda j, rows: left_ref[j - 2, rows, :], lambda i: right_ref[i], v_scr, acc_scr, k_scr)
    for i in range(LEAVES_HERE):
        count = mask_ref[i, 0]
        for t in range(1, SLOTS):
            count = count + mask_ref[i, t]
        diag_ref[:, leaf(i)] = noise_ref[:, leaf(i)] + count.astype(F32)
        part_ref[:, leaf(i)] = diag_ref[:, leaf(i)] * v[:, leaf(i)] + acc_scr[i]


def prepare(parent, mask, packed, skeleton, transfer, noise):
    return call(
        prepare_kernel, [HBM] * 2 + [VMEM] * 4,
        (
            shaped(2, LEAF, 64, dtype=BF16), shaped(2, 64, LEAF, dtype=BF16), shaped(2, 2, RANK, LEAF, dtype=BF16),
            shaped(16, SPAN), shaped(16, 128), shaped(1, SPAN), shaped(TAIL, 128),
        ),
        FLAGS + [
            pltpu.VMEM((4, 32, LEAF), BF16), pltpu.VMEM((2, 16, LEAF), F32), pltpu.VMEM((SLOTS_KEPT, 2, LEAF, LEAF), BF16), pltpu.SemaphoreType.DMA((2,)),
        ],
    )(*off_chip(parent, mask), packed, skeleton, transfer, noise)


def first_kernel(parent_hbm, mask_hbm, before_ref, after_ref, right_ref, part_ref, up_ref, packed_ref, tail_ref,
                 left_out, right_out, local_ref, beside_ref, send_ref, parent_ref, mask_ref, v_scr, acc_scr, k_scr, sems):
    flags = fetch(((parent_hbm, parent_ref), (mask_hbm, mask_ref)), sems)
    for g, ref in enumerate((before_ref, after_ref)):
        left, right = features(ref[:DIM, :])
        for i in range(LEAVES_HERE):
            left_out[2 * g + i] = left[:, leaf(i)].T.astype(BF16)
            right_out[2 * g + i] = right[:, leaf(i)].astype(BF16)
            v_scr[4 * g + i] = halves(ref[DIM:, leaf(i)])
    for i in range(LEAVES_HERE):
        acc_scr[i] = part_ref[:, leaf(i)]
    beside_ref[128:, :] = tail_ref[...]
    for flag in flags:
        flag.wait()
    near_field(6, halo_block, mask_ref, lambda j, rows: left_out[halo_at(j), rows, :], lambda i: right_ref[i],
               v_scr, acc_scr, k_scr)
    local = jnp.concatenate([acc_scr[i] for i in range(LEAVES_HERE)], axis=1)
    local_ref[...] = local
    for n in range(SPAN // 128):
        beside_ref[16 * n : 16 * (n + 1), :] = local[:, 128 * n : 128 * (n + 1)]
    post(parent_ref, up_ref[...], packed_ref[DIM:, :], local, send_ref)


def first(parent, mask, before, after, right, part, up, packed, tail, peers):
    return call(
        first_kernel, [HBM] * 2 + [VMEM] * 7,
        (
            shaped(4, LEAF, 64, dtype=BF16), shaped(4, 64, LEAF, dtype=BF16),
            shaped(16, SPAN), shaped(BESIDE, 128), shaped(peers, ROWS_OUT, 128),
        ),
        FLAGS + [
            pltpu.VMEM((6, 32, LEAF), BF16), pltpu.VMEM((2, 16, LEAF), F32), pltpu.VMEM((SLOTS_KEPT, 2, LEAF, LEAF), BF16), pltpu.SemaphoreType.DMA((2,)),
        ],
    )(*off_chip(parent, mask), before, after, right, part, up, packed, tail)


def across(got, rows):
    return call(across_kernel, [VMEM], (shaped(rows, ROWS_ACROSS, 128),))(got)[0]


def second_kernel(parent_hbm, mask_hbm, coupling_hbm, got_ref, phi_ref, local_ref, packed_ref, diag_ref,
                  before_ref, after_ref, halo_before_ref, halo_after_ref, left_ref, right_ref,
                  halo_left_ref, halo_right_ref,
                  residual_ref, along_ref, kept_ref, out_ref, send_ref,
                  parent_ref, mask_ref, coupling_scr, img_scr, v_scr, acc_scr, k_scr, bt_scr, sems):
    copies = fetch(((coupling_hbm, coupling_scr), (parent_hbm, parent_ref), (mask_hbm, mask_ref)), sems)
    sides = ((halo_before_ref, before_ref), (halo_after_ref, after_ref))
    for g, (msg_ref, _) in enumerate(sides):
        sk_left, _ = features(msg_ref[192:200, :])
        for i in range(LEAVES_HERE):
            rows = sk_left[:, RANK * i : RANK * (i + 1)].T.astype(BF16)
            bt = matern(rows, halo_right_ref[2 * g + i]) * (1.0 / math.sqrt(LEAF))
            bt_scr[2 * g + i, 0], bt_scr[2 * g + i, 1] = pair(bt)
    norm, inner = coupled_image(got_ref, coupling_scr, img_scr, copies[0].wait)
    step = norm / inner
    copies[1].wait()
    copies[2].wait()
    rhs = packed_ref[DIM:, :]
    along = local_ref[...] + own_far(parent_ref, phi_ref, img_scr)
    residual = rhs - step * along
    along_ref[...] = along
    residual_ref[...] = residual
    lane = lax.broadcasted_iota(jnp.int32, (16, 128), 1)
    kept_ref[...] = jnp.where(lane == 0, norm, jnp.where(lane == 1, step, 0.0))
    for i in range(LEAVES_HERE):
        v_scr[2 + i] = halves(residual[:, leaf(i)])
    for g, (msg_ref, ref) in enumerate(sides):
        for i in range(LEAVES_HERE):
            parent = jnp.max(msg_ref[200:208, RANK * i : RANK * (i + 1)]).astype(jnp.int32)
            moved = msg_ref[128:192, RANK * i : RANK * (i + 1)].astype(BF16)
            pushed = jnp.zeros((16, RANK), F32)
            parts = lax.dot_general(
                jnp.concatenate(split(img_scr[parent], 3), axis=0).astype(BF16), moved, (((1,), (1,)), ((), ())),
                preferred_element_type=F32,
            )
            pushed = parts[:16] + parts[16:32] + parts[32:]
            far = pair_dot(pushed, bt_scr[2 * g + i, 0], bt_scr[2 * g + i, 1])
            local = jnp.concatenate([msg_ref[16 * n : 16 * (n + 1), :] for n in range(4 * i, 4 * (i + 1))], axis=1)
            v_scr[4 * g + i] = halves(ref[DIM:, leaf(i)] - step * (local + far))
    up = lifted(residual, phi_ref)
    acc_scr[...] = jnp.zeros(acc_scr.shape, F32)
    near_field(4, own_block, mask_ref, lambda j, rows: left_ref[j - 2, rows, :], lambda i: right_ref[i], v_scr, acc_scr, k_scr)
    near_field(6, halo_block, mask_ref, lambda j, rows: halo_left_ref[halo_at(j), rows, :], lambda i: right_ref[i],
               v_scr, acc_scr, k_scr)
    near = jnp.concatenate([acc_scr[i] for i in range(LEAVES_HERE)], axis=1)
    local = diag_ref[...] * residual + near
    out_ref[...] = local
    post(parent_ref, up, residual, local, send_ref)


def second(parent, mask, coupling, *arrays, peers):
    return call(
        second_kernel, [HBM] * 3 + [VMEM] * len(arrays),
        (
            shaped(16, SPAN), shaped(16, SPAN), shaped(16, 128), shaped(16, SPAN), shaped(peers, ROWS_OUT, 128),
        ),
        FLAGS + [
            pltpu.VMEM((LEVELS * RANK, LEVELS * RANK), BF16),
            pltpu.VMEM((LEVELS, 16, RANK), F32), pltpu.VMEM((6, 32, LEAF), BF16), pltpu.VMEM((2, 16, LEAF), F32), pltpu.VMEM((SLOTS_KEPT, 2, LEAF, LEAF), BF16),
            pltpu.VMEM((4, 2, RANK, LEAF), BF16), pltpu.SemaphoreType.DMA((3,)),
        ],
    )(*off_chip(parent, mask, coupling), *arrays)


def last_kernel(parent_hbm, coupling_ref, got_ref, phi_ref, local_ref, packed_ref, residual_ref, along_ref, kept_ref,
                solution_ref, out_ref, parent_ref, img_scr, sems):
    flags = fetch(((parent_hbm, parent_ref),), sems)
    norm, inner = coupled_image(got_ref, coupling_ref, img_scr)
    before = kept_ref[:, 0:1]
    first_step = kept_ref[:, 1:2]
    growth = norm / before
    step = norm / (inner - growth * norm / first_step)
    rhs = packed_ref[DIM:, :]
    residual = residual_ref[...]
    solution_ref[...] = first_step * rhs + step * (residual + growth * rhs)
    flags[0].wait()
    applied = local_ref[...] + own_far(parent_ref, phi_ref, img_scr)
    out_ref[...] = residual - step * (applied + growth * along_ref[...])


def last(parent, *arrays):
    return call(
        last_kernel, [HBM] + [VMEM] * len(arrays), (shaped(16, SPAN), shaped(16, SPAN)),
        (FLAGS[0], pltpu.VMEM((LEVELS, 16, RANK), F32), pltpu.SemaphoreType.DMA((1,))),
    )(*off_chip(parent), *arrays)


def beside(x):
    count = lax.axis_size(AXES)
    before = lax.ppermute(x, AXES, [(i, i + 1) for i in range(count - 1)])
    after = lax.ppermute(x, AXES, [(i + 1, i) for i in range(count - 1)])
    return before, after


def exchange(send, *ready):
    row = lax.all_to_all(send, ("z", "c"), 0, 0, tiled=True)
    column, *ready = lax.optimization_barrier((across(row, lax.axis_size("y")), *ready))
    return lax.all_to_all(column, "y", 0, 0, tiled=True), *ready


def per_device(coords, skeleton, transfer, coupling, parent, near_mask, noise, rhs):
    peers = lax.axis_size(("z", "c"))
    packed, skeleton, transfer, noise = pack(coords, skeleton, transfer, noise.reshape(1, SPAN), rhs)
    before, after = beside(packed)
    left, right, phi, part, up, diag, tail = prepare(parent, near_mask, packed, skeleton, transfer, noise)
    halo_left, halo_right, local, message, send = first(
        parent, near_mask, before, after, right, part, up, packed, tail, peers
    )
    halo_before, halo_after = beside(message)
    got, halo_before, halo_after = exchange(send, halo_before, halo_after)
    residual, along, kept, local, send = second(
        parent, near_mask, coupling, got, phi, local, packed, diag, before, after,
        halo_before, halo_after, left, right, halo_left, halo_right, peers=peers,
    )
    (got,) = exchange(send)
    return last(parent, coupling, got, phi, local, packed, residual, along, kept)


def solution(mesh):
    finer = Mesh(mesh.devices.reshape(8, 8, 2, mesh.shape["rep"]), (*AXES, "rep"))
    placed = (
        P(None, AXES),
        P(None, AXES),
        P(AXES, None, None),
        P(),
        P(AXES),
        P(AXES, None),
        P(AXES),
        P("rep", AXES),
    )
    return jax.shard_map(
        per_device,
        mesh=finer,
        in_specs=placed,
        out_specs=(P("rep", AXES), P("rep", AXES)),
        check_vma=False,
    )
```

```python
import math

import jax
import jax.numpy as jnp
from jax import lax
from jax.experimental import pallas as pl
from jax.experimental.pallas import tpu as pltpu
from jax.sharding import Mesh
from jax.sharding import PartitionSpec as P


LEAF = 512
DIM = 8
RANK = 64
LEVELS = 16
LEAVES_HERE = 2
SLOTS = 5
SPAN = LEAVES_HERE * LEAF
AXES = ("y", "z", "c")
SCALE = math.sqrt(3.0) / 4.0
LOG2E = 1.4426950408889634
CHUNK = 64
SLOTS_KEPT = 2
F32 = jnp.float32
BF16 = jnp.bfloat16


def split(x, parts):
    out = []
    for _ in range(parts):
        piece = x.astype(BF16).astype(F32)
        out.append(piece)
        x = x - piece
    return out


def pair(x):
    hi, lo = split(x, 2)
    return hi.astype(BF16), lo.astype(BF16)


def pair_dot(x, hi, lo, contract=0):
    dims = (((1,), (contract,)), ((), ()))
    xh, xl = split(x, 2)
    both = jnp.concatenate([xh, xl], axis=0).astype(BF16)
    wide = lax.dot_general(both, hi, dims, preferred_element_type=F32)
    low = lax.dot_general(xh.astype(BF16), lo, dims, preferred_element_type=F32)
    return wide[:16] + wide[16:] + low


def features(c):
    n = c.shape[1]
    c = c * SCALE
    p1, p2, p3 = split(c, 3)
    n1, n2, n3 = split(jnp.sum(c * c, axis=0, keepdims=True), 3)
    row = lax.broadcasted_iota(jnp.int32, (8, n), 0)
    def pick(*rows):
        out = jnp.zeros((8, n), F32)
        for at, value in rows:
            out = jnp.where(row == at, value, out)
        return out
    left_norm = pick((0, n1), (1, n2), (2, n3), (3, 1.0), (4, 1.0), (5, 1.0))
    right_norm = pick((0, 1.0), (1, 1.0), (2, 1.0), (3, n1), (4, n2), (5, n3))
    none = jnp.zeros((8, n), F32)
    q1, q2, q3 = -2.0 * p1, -2.0 * p2, -2.0 * p3
    left = jnp.concatenate([p1, p1, p2, p2, p1, p3, left_norm, none], axis=0)
    right = jnp.concatenate([q1, q2, q1, q2, q3, q1, right_norm, none], axis=0)
    return left, right


def matern(left, right):
    d2 = jnp.dot(left, right, preferred_element_type=F32)
    d2 = jnp.maximum(d2, 1e-30)
    s = d2 * lax.rsqrt(d2)
    return (1.0 + s) * jnp.exp2(s * -LOG2E)


VMEM = pl.BlockSpec(memory_space=pltpu.VMEM)
SMEM = pl.BlockSpec(memory_space=pltpu.SMEM)
HBM = pl.BlockSpec(memory_space=pltpu.HBM)
LIMIT = 24 * 1024 * 1024
PAIRS = 4
ROWS_OUT = 24
ROWS_ACROSS = 8 * PAIRS + 8
TAIL = 80
BESIDE = 128 + TAIL


def off_chip(*arrays):
    return [pltpu.with_memory_space_constraint(x, pltpu.HBM) for x in arrays]


def shaped(*dims, dtype=F32):
    return jax.ShapeDtypeStruct(dims, dtype)


def call(kernel, in_specs, outs, scratch=()):
    return pl.pallas_call(
        kernel,
        out_shape=tuple(outs),
        in_specs=in_specs,
        out_specs=tuple(VMEM for _ in outs),
        scratch_shapes=list(scratch),
        compiler_params=pltpu.CompilerParams(vmem_limit_bytes=LIMIT),
    )


def leaf(i):
    return slice(LEAF * i, LEAF * (i + 1))


def halves(x):
    hi, lo = split(x * (1.0 / LEAF), 2)
    return jnp.concatenate([hi, lo], axis=0).astype(BF16)


def own_block(b):
    i = b // 2
    return i, 2 + b % 2


def halo_at(j):
    return j - 2 * ((j >= 4) * 1)


def halo_block(b):
    i = b // 3
    m = i + b % 3
    far = (m >= 2) * 1
    return i, m + 2 * far


def near_field(count, place, mask_ref, left_of, right_of, v_scr, acc_scr, k_scr):
    for b in range(count):
        i, j = place(b)
        slot = b % SLOTS_KEPT
        right = right_of(i)
        for h in range(LEAF // CHUNK):
            rows = slice(CHUNK * h, CHUNK * (h + 1))
            k = matern(left_of(j, rows), right)
            kh = k.astype(BF16)
            k_scr[slot, 0, rows, :] = kh
            k_scr[slot, 1, rows, :] = (k - kh.astype(F32)).astype(BF16)
        v = v_scr[j]
        total = jnp.dot(v, k_scr[slot, 0], preferred_element_type=F32)
        low = jnp.dot(v[:16], k_scr[slot, 1], preferred_element_type=F32)
        acc_scr[i] = acc_scr[i] + mask_ref[i, j - i].astype(F32) * (total[:16] + total[16:] + low)


def fetch(pairs, sems):
    copies = [pltpu.make_async_copy(src, dst, sems.at[n]) for n, (src, dst) in enumerate(pairs)]
    for copy in copies:
        copy.start()
    return copies


def lifted(v, phi_ref):
    return jnp.concatenate(
        [pair_dot(v[:, leaf(i)], phi_ref[i, 0], phi_ref[i, 1], contract=1) for i in range(LEAVES_HERE)], axis=1
    )


def post(parent_ref, up, v, local, send_ref):
    lane = lax.broadcasted_iota(jnp.int32, (8, 128), 1)
    norm = jnp.sum(v * v, axis=1, keepdims=True)
    inner = jnp.sum(v * local, axis=1, keepdims=True)
    tile = jnp.zeros((8, 128), F32)
    for at, value in enumerate(
        (norm[:8], inner[:8], norm[8:], inner[8:], parent_ref[0].astype(F32), parent_ref[1].astype(F32))
    ):
        tile = jnp.where(lane == at, value, tile)
    for d in range(send_ref.shape[0]):
        send_ref[d, :16, :] = up
        send_ref[d, 16:, :] = tile


def paired(tiles):
    lane = lax.broadcasted_iota(jnp.int32, (16, 128), 1)
    whole = [t + pltpu.roll(t, 64, axis=1) for t in tiles]
    return [jnp.where(lane < 64, whole[m], whole[m + 1]) for m in range(0, len(tiles), 2)]


def across_kernel(got_ref, send_ref):
    offset = (PAIRS * lax.axis_index("c")).astype(F32)
    lane = lax.broadcasted_iota(jnp.int32, (1, 128), 1)
    first = got_ref[0, 16:17, 4:5]
    begin = first + offset
    tiles = [jnp.zeros((16, 128), F32) for _ in range(PAIRS)]
    scalars = jnp.zeros((8, 128), F32)
    for d in range(got_ref.shape[0]):
        slot = jnp.where(lane < 64, got_ref[d, 16:17, 4:5], got_ref[d, 16:17, 5:6]) - begin
        piece = got_ref[d, :16, :]
        for s in range(PAIRS):
            tiles[s] = tiles[s] + jnp.where(slot == float(s), piece, 0.0)
        scalars = scalars + got_ref[d, 16:, :]
    scalars = jnp.where(lane == 4, first, scalars)
    tiles = paired(tiles)
    for y in range(send_ref.shape[0]):
        for k in range(PAIRS // 2):
            send_ref[y, 16 * k : 16 * (k + 1), :] = tiles[k]
        send_ref[y, 8 * PAIRS :, :] = scalars


def whole_sums(got_ref):
    lane = lax.broadcasted_iota(jnp.int32, (1, 128), 1)
    half = (lane >= 64).astype(F32)
    tiles = [jnp.zeros((16, 128), F32) for _ in range(LEVELS)]
    scalars = jnp.zeros((8, 128), F32)
    for y in range(got_ref.shape[1]):
        first = got_ref[0, y, 8 * PAIRS : 8 * PAIRS + 1, 4:5] + half
        for c in range(got_ref.shape[0]):
            for k in range(PAIRS // 2):
                piece = got_ref[c, y, 16 * k : 16 * (k + 1), :]
                cluster = first + float(PAIRS * c + 2 * k)
                for q in range(LEVELS):
                    tiles[q] = tiles[q] + jnp.where(cluster == float(q), piece, 0.0)
        scalars = scalars + got_ref[0, y, 8 * PAIRS :, :]
    norm = jnp.concatenate([scalars[:, 0:1], scalars[:, 2:3]], axis=0)
    inner = jnp.concatenate([scalars[:, 1:2], scalars[:, 3:4]], axis=0)
    return jnp.concatenate(paired(tiles), axis=1), norm, inner


def coupled_image(got_ref, coupling_ref, img_scr, ready=lambda: None):
    sums, norm, inner = whole_sums(got_ref)
    parts = jnp.concatenate(split(sums, 3), axis=0).astype(BF16)
    ready()
    image = jnp.dot(parts, coupling_ref[...], preferred_element_type=F32)
    image = image[:16] + image[16:32] + image[32:]
    inner = inner + jnp.sum(sums * image, axis=1, keepdims=True)
    for p in range(LEVELS):
        img_scr[p] = image[:, RANK * p : RANK * (p + 1)]
    return norm, inner


def own_far(parent_ref, phi_ref, img_scr):
    return jnp.concatenate(
        [pair_dot(img_scr[parent_ref[i]], phi_ref[i, 0], phi_ref[i, 1]) for i in range(LEAVES_HERE)], axis=1
    )


def pack_kernel(coords_hbm, skeleton_hbm, transfer_hbm, noise_hbm, rhs_hbm, packed_ref, skeleton_ref, transfer_ref,
                noise_ref, sems):
    for copy in fetch(
        (
            (rhs_hbm, packed_ref.at[pl.ds(DIM, 16), :]), (coords_hbm, packed_ref.at[pl.ds(0, DIM), :]),
            (transfer_hbm, transfer_ref), (skeleton_hbm, skeleton_ref), (noise_hbm, noise_ref),
        ),
        sems,
    ):
        copy.wait()


def pack(coords, skeleton, transfer, noise, rhs):
    return call(
        pack_kernel, [HBM] * 5,
        (shaped(24, SPAN), shaped(DIM, 128), shaped(2, RANK, RANK, dtype=BF16), shaped(1, SPAN)),
        (pltpu.SemaphoreType.DMA((5,)),),
    )(*off_chip(coords, skeleton, transfer, noise, rhs))


FLAGS = [pltpu.SMEM((2,), jnp.int32), pltpu.SMEM((2, SLOTS), jnp.int32)]


def prepare_kernel(parent_hbm, mask_hbm, packed_ref, skeleton_ref, transfer_ref, noise_ref,
                   left_ref, right_ref, phi_ref, part_ref, up_ref, diag_ref, tail_ref,
                   parent_ref, mask_ref, v_scr, acc_scr, k_scr, sems):
    flags = fetch(((parent_hbm, parent_ref), (mask_hbm, mask_ref)), sems)
    left, right = features(packed_ref[:DIM, :])
    v = packed_ref[DIM:, :]
    for i in range(LEAVES_HERE):
        left_ref[i] = left[:, leaf(i)].T.astype(BF16)
        right_ref[i] = right[:, leaf(i)].astype(BF16)
        v_scr[2 + i] = halves(v[:, leaf(i)])
    skeleton = skeleton_ref[...]
    sk_left, _ = features(skeleton)
    for i in range(LEAVES_HERE):
        rows = sk_left[:, RANK * i : RANK * (i + 1)].T.astype(BF16)
        bt = matern(rows, right_ref[i]) * (1.0 / math.sqrt(LEAF))
        moved = transfer_ref[i]
        phi = jnp.zeros((RANK, LEAF), F32)
        for part in split(bt, 3):
            phi = phi + lax.dot_general(
                moved, part.astype(BF16), (((0,), (0,)), ((), ())), preferred_element_type=F32
            )
        phi_ref[i, 0], phi_ref[i, 1] = pair(phi)
    tail_ref[:64, :] = jnp.concatenate([transfer_ref[i].astype(F32) for i in range(LEAVES_HERE)], axis=1)
    tail_ref[64:72, :] = skeleton
    up_ref[...] = lifted(v, phi_ref)
    acc_scr[...] = jnp.zeros(acc_scr.shape, F32)
    for flag in flags:
        flag.wait()
    lane = lax.broadcasted_iota(jnp.int32, (8, 128), 1)
    tail_ref[72:, :] = jnp.where(lane < 64, parent_ref[0].astype(F32), parent_ref[1].astype(F32))
    near_field(4, own_block, mask_ref, lambda j, rows: left_ref[j - 2, rows, :], lambda i: right_ref[i], v_scr, acc_scr, k_scr)
    for i in range(LEAVES_HERE):
        count = mask_ref[i, 0]
        for t in range(1, SLOTS):
            count = count + mask_ref[i, t]
        diag_ref[:, leaf(i)] = noise_ref[:, leaf(i)] + count.astype(F32)
        part_ref[:, leaf(i)] = diag_ref[:, leaf(i)] * v[:, leaf(i)] + acc_scr[i]


def prepare(parent, mask, packed, skeleton, transfer, noise):
    return call(
        prepare_kernel, [HBM] * 2 + [VMEM] * 4,
        (
            shaped(2, LEAF, 64, dtype=BF16), shaped(2, 64, LEAF, dtype=BF16), shaped(2, 2, RANK, LEAF, dtype=BF16),
            shaped(16, SPAN), shaped(16, 128), shaped(1, SPAN), shaped(TAIL, 128),
        ),
        FLAGS + [
            pltpu.VMEM((4, 32, LEAF), BF16), pltpu.VMEM((2, 16, LEAF), F32), pltpu.VMEM((SLOTS_KEPT, 2, LEAF, LEAF), BF16), pltpu.SemaphoreType.DMA((2,)),
        ],
    )(*off_chip(parent, mask), packed, skeleton, transfer, noise)


def first_kernel(parent_hbm, mask_hbm, partner_ref, cross_ref, right_ref, part_ref, up_ref, packed_ref, tail_ref,
                 left_out, right_out, local_ref, beside_ref, send_ref, parent_ref, mask_ref, v_scr, acc_scr, k_scr, sems):
    flags = fetch(((parent_hbm, parent_ref), (mask_hbm, mask_ref)), sems)
    for g, beyond in enumerate(ordered(partner_ref[...], cross_ref[...])):
        left, right = features(beyond[:DIM, :])
        for i in range(LEAVES_HERE):
            left_out[2 * g + i] = left[:, leaf(i)].T.astype(BF16)
            right_out[2 * g + i] = right[:, leaf(i)].astype(BF16)
            v_scr[4 * g + i] = halves(beyond[DIM:, leaf(i)])
    for i in range(LEAVES_HERE):
        acc_scr[i] = part_ref[:, leaf(i)]
    beside_ref[128:, :] = tail_ref[...]
    for flag in flags:
        flag.wait()
    near_field(6, halo_block, mask_ref, lambda j, rows: left_out[halo_at(j), rows, :], lambda i: right_ref[i],
               v_scr, acc_scr, k_scr)
    local = jnp.concatenate([acc_scr[i] for i in range(LEAVES_HERE)], axis=1)
    local_ref[...] = local
    for n in range(SPAN // 128):
        beside_ref[16 * n : 16 * (n + 1), :] = local[:, 128 * n : 128 * (n + 1)]
    post(parent_ref, up_ref[...], packed_ref[DIM:, :], local, send_ref)


def first(parent, mask, partner, cross, right, part, up, packed, tail, peers):
    return call(
        first_kernel, [HBM] * 2 + [VMEM] * 7,
        (
            shaped(4, LEAF, 64, dtype=BF16), shaped(4, 64, LEAF, dtype=BF16),
            shaped(16, SPAN), shaped(BESIDE, 128), shaped(peers, ROWS_OUT, 128),
        ),
        FLAGS + [
            pltpu.VMEM((6, 32, LEAF), BF16), pltpu.VMEM((2, 16, LEAF), F32), pltpu.VMEM((SLOTS_KEPT, 2, LEAF, LEAF), BF16), pltpu.SemaphoreType.DMA((2,)),
        ],
    )(*off_chip(parent, mask), partner, cross, right, part, up, packed, tail)


def across(got, rows):
    return call(across_kernel, [VMEM], (shaped(rows, ROWS_ACROSS, 128),))(got)[0]


def second_kernel(parent_hbm, mask_hbm, coupling_hbm, got_ref, phi_ref, local_ref, packed_ref, diag_ref,
                  partner_ref, cross_ref, partner_msg_ref, cross_msg_ref, left_ref, right_ref,
                  halo_left_ref, halo_right_ref,
                  residual_ref, along_ref, kept_ref, out_ref, send_ref,
                  parent_ref, mask_ref, coupling_scr, img_scr, v_scr, acc_scr, k_scr, bt_scr, sems):
    copies = fetch(((coupling_hbm, coupling_scr), (parent_hbm, parent_ref), (mask_hbm, mask_ref)), sems)
    messages = ordered(partner_msg_ref[...], cross_msg_ref[...])
    beyond = ordered(partner_ref[DIM:, :], cross_ref[DIM:, :])
    for g, msg in enumerate(messages):
        sk_left, _ = features(msg[192:200, :])
        for i in range(LEAVES_HERE):
            rows = sk_left[:, RANK * i : RANK * (i + 1)].T.astype(BF16)
            bt = matern(rows, halo_right_ref[2 * g + i]) * (1.0 / math.sqrt(LEAF))
            bt_scr[2 * g + i, 0], bt_scr[2 * g + i, 1] = pair(bt)
    norm, inner = coupled_image(got_ref, coupling_scr, img_scr, copies[0].wait)
    step = norm / inner
    copies[1].wait()
    copies[2].wait()
    rhs = packed_ref[DIM:, :]
    along = local_ref[...] + own_far(parent_ref, phi_ref, img_scr)
    residual = rhs - step * along
    along_ref[...] = along
    residual_ref[...] = residual
    lane = lax.broadcasted_iota(jnp.int32, (16, 128), 1)
    kept_ref[...] = jnp.where(lane == 0, norm, jnp.where(lane == 1, step, 0.0))
    for i in range(LEAVES_HERE):
        v_scr[2 + i] = halves(residual[:, leaf(i)])
    for g, msg in enumerate(messages):
        for i in range(LEAVES_HERE):
            parent = jnp.max(msg[200:208, RANK * i : RANK * (i + 1)]).astype(jnp.int32)
            moved = msg[128:192, RANK * i : RANK * (i + 1)].astype(BF16)
            pushed = jnp.zeros((16, RANK), F32)
            parts = lax.dot_general(
                jnp.concatenate(split(img_scr[parent], 3), axis=0).astype(BF16), moved, (((1,), (1,)), ((), ())),
                preferred_element_type=F32,
            )
            pushed = parts[:16] + parts[16:32] + parts[32:]
            far = pair_dot(pushed, bt_scr[2 * g + i, 0], bt_scr[2 * g + i, 1])
            local = jnp.concatenate([msg[16 * n : 16 * (n + 1), :] for n in range(4 * i, 4 * (i + 1))], axis=1)
            v_scr[4 * g + i] = halves(beyond[g][:, leaf(i)] - step * (local + far))
    up = lifted(residual, phi_ref)
    acc_scr[...] = jnp.zeros(acc_scr.shape, F32)
    near_field(4, own_block, mask_ref, lambda j, rows: left_ref[j - 2, rows, :], lambda i: right_ref[i], v_scr, acc_scr, k_scr)
    near_field(6, halo_block, mask_ref, lambda j, rows: halo_left_ref[halo_at(j), rows, :], lambda i: right_ref[i],
               v_scr, acc_scr, k_scr)
    near = jnp.concatenate([acc_scr[i] for i in range(LEAVES_HERE)], axis=1)
    local = diag_ref[...] * residual + near
    out_ref[...] = local
    post(parent_ref, up, residual, local, send_ref)


def second(parent, mask, coupling, *arrays, peers):
    return call(
        second_kernel, [HBM] * 3 + [VMEM] * len(arrays),
        (
            shaped(16, SPAN), shaped(16, SPAN), shaped(16, 128), shaped(16, SPAN), shaped(peers, ROWS_OUT, 128),
        ),
        FLAGS + [
            pltpu.VMEM((LEVELS * RANK, LEVELS * RANK), BF16),
            pltpu.VMEM((LEVELS, 16, RANK), F32), pltpu.VMEM((6, 32, LEAF), BF16), pltpu.VMEM((2, 16, LEAF), F32), pltpu.VMEM((SLOTS_KEPT, 2, LEAF, LEAF), BF16),
            pltpu.VMEM((4, 2, RANK, LEAF), BF16), pltpu.SemaphoreType.DMA((3,)),
        ],
    )(*off_chip(parent, mask, coupling), *arrays)


def last_kernel(parent_hbm, coupling_ref, got_ref, phi_ref, local_ref, packed_ref, residual_ref, along_ref, kept_ref,
                solution_ref, out_ref, parent_ref, img_scr, sems):
    flags = fetch(((parent_hbm, parent_ref),), sems)
    norm, inner = coupled_image(got_ref, coupling_ref, img_scr)
    before = kept_ref[:, 0:1]
    first_step = kept_ref[:, 1:2]
    growth = norm / before
    step = norm / (inner - growth * norm / first_step)
    rhs = packed_ref[DIM:, :]
    residual = residual_ref[...]
    solution_ref[...] = first_step * rhs + step * (residual + growth * rhs)
    flags[0].wait()
    applied = local_ref[...] + own_far(parent_ref, phi_ref, img_scr)
    out_ref[...] = residual - step * (applied + growth * along_ref[...])


def last(parent, *arrays):
    return call(
        last_kernel, [HBM] + [VMEM] * len(arrays), (shaped(16, SPAN), shaped(16, SPAN)),
        (FLAGS[0], pltpu.VMEM((LEVELS, 16, RANK), F32), pltpu.SemaphoreType.DMA((1,))),
    )(*off_chip(parent), *arrays)


def beside(x):
    count = lax.axis_size(AXES)
    swaps = [(i, i ^ 1) for i in range(count)]
    crossings = [(i, i + 1 if i % 2 else i - 1) for i in range(1, count - 1)]
    cross = lax.ppermute(x, AXES, crossings)
    return lax.ppermute(x, AXES, swaps), cross


def ordered(partner, cross):
    core = lax.axis_index("c")
    return jnp.where(core == 0, cross, partner), jnp.where(core == 0, partner, cross)


def exchange(send, *ready):
    row = lax.all_to_all(send, ("z", "c"), 0, 0, tiled=True)
    column, *ready = lax.optimization_barrier((across(row, lax.axis_size("y")), *ready))
    return lax.all_gather(lax.all_to_all(column, "y", 0, 0, tiled=True), "c"), *ready


def per_device(coords, skeleton, transfer, coupling, parent, near_mask, noise, rhs):
    peers = lax.axis_size(("z", "c"))
    packed, skeleton, transfer, noise = pack(coords, skeleton, transfer, noise.reshape(1, SPAN), rhs)
    partner, cross = beside(packed)
    left, right, phi, part, up, diag, tail = prepare(parent, near_mask, packed, skeleton, transfer, noise)
    halo_left, halo_right, local, message, send = first(
        parent, near_mask, partner, cross, right, part, up, packed, tail, peers
    )
    partner_msg, cross_msg = beside(message)
    got, partner_msg, cross_msg = exchange(send, partner_msg, cross_msg)
    residual, along, kept, local, send = second(
        parent, near_mask, coupling, got, phi, local, packed, diag, partner, cross,
        partner_msg, cross_msg, left, right, halo_left, halo_right, peers=peers,
    )
    (got,) = exchange(send)
    return last(parent, coupling, got, phi, local, packed, residual, along, kept)


def solution(mesh):
    finer = Mesh(mesh.devices.reshape(8, 8, 2, mesh.shape["rep"]), (*AXES, "rep"))
    placed = (
        P(None, AXES),
        P(None, AXES),
        P(AXES, None, None),
        P(),
        P(AXES),
        P(AXES, None),
        P(AXES),
        P("rep", AXES),
    )
    return jax.shard_map(
        per_device,
        mesh=finer,
        in_specs=placed,
        out_specs=(P("rep", AXES), P("rep", AXES)),
        check_vma=False,
    )
```
